32 devices in a mesh: gx: 4 (over y, core), gy: 8 (over z, x).
Axes of the slice: x: 2, y: 2, z: 4, core: 2. Of those that a mesh axis runs over, the one named last changes fastest.
Arguments:
- previous: float32 [2, 7, 512, 1024], P(None, None, 'gx', 'gy'), may hold values from -6 to 6
- dissipated: float32 [2, 4, 512, 1024], P(None, None, 'gx', 'gy'), may hold values from 0.05 to 3
- material: int32 [4, 512, 1024], P(None, 'gx', 'gy'), may hold values from 0 to 3
- coolant: int32 [3, 512, 1024], P(None, 'gx', 'gy'), may hold values from 0 to 3
Outputs:
- temperature: float32 [2, 7, 512, 1024], P(None, None, 'gx', 'gy')
The draws below stay inside these ranges and needn't reach their ends.
All inputs are finite; a program needn't handle non-finite values.
Results may differ from the reference program's by a relative error of at most 0.00011.
Values sent between devices are 32-bit elements; how exact they have to be, the bound alone decides.
A program may use at most 64 MiB of HBM per device.

```python
import math
import jax
import jax.numpy as jnp
from jax import lax

TIERS = 4
CHANNELS = 3
LAYERS = 7
SCEN = 2
ITERS = 3
NX = 512
NY = 1024


def set_ends(entries, stream_key, low, largest):
    longest = entries.shape.index(max(entries.shape))
    spots = []
    for shift in (0, 1):
        where = [jax.random.randint(jax.random.fold_in(stream_key, axis), (), 0, length) for axis, length in enumerate(entries.shape)]
        where[longest] = (where[longest] + shift) % entries.shape[longest]
        spots.append(tuple(where))
    return entries.at[spots[0]].set(low).at[spots[1]].set(largest)


def block_scale(key, dims, split, low, largest):
    def one(position, shards_of):
        steps = jax.random.uniform(jax.random.fold_in(jax.random.fold_in(key, 6), position), (shards_of,), jnp.float32, low / len(split), largest / len(split))
        return jnp.repeat(jnp.exp(steps), dims[position] // shards_of).reshape((-1,) + (1,) * (len(dims) - position - 1))

    level = one(*split[0])
    for cut in split[1:]:
        level = level * one(*cut)
    return level


def bell_draw(key, shape, deviation, bound, cuts=(), dtype=jnp.bfloat16):
    result = jax.random.normal(key, shape, jnp.float32) * deviation
    if len(cuts) > 0:
        result = block_scale(key, shape, cuts, -0.22, 0.18) * result
    return jnp.clip(result, min=-bound, max=bound).astype(dtype)


def setup_inputs(seed: int = 0) -> dict:
    streams_of = jax.random.split(jax.random.key(seed), 5)
    previous = bell_draw(streams_of[0], (SCEN, LAYERS, NX, NY), 1.0, 6.0, ((2, 4), (3, 8)), jnp.float32)
    dissipated = jnp.clip(jnp.exp(math.log(3.0) - 4.0943445 * jax.random.uniform(streams_of[1], (SCEN, TIERS, NX, NY), jnp.float32) ** block_scale(streams_of[1], (SCEN, TIERS, NX, NY), ((2, 4), (3, 8)), -0.2, 0.2)), 0.05, 3.0)
    material = set_ends(jax.random.randint(streams_of[2], (TIERS, NX, NY), 0, 4), jax.random.fold_in(streams_of[2], 1), 0, 3).astype(jnp.int32)
    coolant = set_ends(jax.random.randint(streams_of[3], (CHANNELS, NX, NY), 0, 4), jax.random.fold_in(streams_of[3], 1), 0, 3).astype(jnp.int32)
    return dict(previous=previous, dissipated=dissipated, material=material, coolant=coolant)


TIER_K = (1.0, 0.3, 0.12, 2.5)
CHANNEL_K = (1.0, 0.3, 0.25, 0.2)
CHANNEL_SINK = (0.0, 0.15, 0.45, 1.2)
TIER_HEAT = 0.05
CHANNEL_HEAT = 0.2
VERTICAL = 4.0

def lookup(codes, table):
    total = jnp.zeros(codes.shape, jnp.float32)
    for index, value in enumerate(table):
        total = total + jnp.where(codes == index, jnp.float32(value), jnp.float32(0.0))
    return total

def mix(tiers, channels):
    rows = []
    for layer in range(2 * tiers.shape[0] - 1):
        rows.append(tiers[layer // 2] if layer % 2 == 0 else channels[layer // 2])
    return jnp.stack(rows)

def capacity_column(layers):
    return jnp.array([TIER_HEAT if layer % 2 == 0 else CHANNEL_HEAT for layer in range(layers)], jnp.float32)

def couplings(padded_k):
    centre = padded_k[:, 1:-1, 1:-1]
    g_north = jnp.sqrt(centre * padded_k[:, :-2, 1:-1])
    g_south = jnp.sqrt(centre * padded_k[:, 2:, 1:-1])
    g_west = jnp.sqrt(centre * padded_k[:, 1:-1, :-2])
    g_east = jnp.sqrt(centre * padded_k[:, 1:-1, 2:])
    g_vertical = VERTICAL * jnp.sqrt(centre[:-1] * centre[1:])
    return (g_north, g_south, g_west, g_east, g_vertical)

def operate(padded_v, padded_k, sink, capacity):
    g_north, g_south, g_west, g_east, g_vertical = couplings(padded_k)
    centre = padded_v[:, 1:-1, 1:-1]
    lateral = g_north * (centre - padded_v[:, :-2, 1:-1]) + g_south * (centre - padded_v[:, 2:, 1:-1])
    lateral = lateral + g_west * (centre - padded_v[:, 1:-1, :-2]) + g_east * (centre - padded_v[:, 1:-1, 2:])
    flux = g_vertical * (centre[:-1] - centre[1:])
    zero_row = jnp.zeros_like(centre[:1])
    vertical = jnp.concatenate([flux, zero_row], 0) - jnp.concatenate([zero_row, flux], 0)
    return (capacity + sink) * centre + lateral + vertical

def diagonal_terms(padded_k, sink, capacity):
    g_north, g_south, g_west, g_east, g_vertical = couplings(padded_k)
    zero_row = jnp.zeros_like(g_vertical[:1])
    vertical = jnp.concatenate([g_vertical, zero_row], 0) + jnp.concatenate([zero_row, g_vertical], 0)
    return capacity + sink + g_north + g_south + g_west + g_east + vertical

def padded(field):
    return jnp.pad(field, ((0, 0), (1, 1), (1, 1)))

def reference(previous, dissipated, material, coolant):
    tier_k = lookup(material, TIER_K)
    kappa = mix(tier_k, lookup(coolant, CHANNEL_K))
    sink = mix(jnp.zeros_like(tier_k), lookup(coolant, CHANNEL_SINK))
    capacity = capacity_column(kappa.shape[0])[:, None, None]
    padded_k = padded(kappa)
    diagonal = diagonal_terms(padded_k, sink, capacity)

    def solve_one(pair):
        start, heat = pair
        source = capacity * start + mix(heat, jnp.zeros_like(heat[:-1]))
        residual = source - operate(padded(start), padded_k, sink, capacity)
        solution = start
        scaled = residual / diagonal
        norm_now = jnp.sum(residual * scaled)
        direction = scaled
        for iteration in range(ITERS):
            image = operate(padded(direction), padded_k, sink, capacity)
            step_size = norm_now / jnp.sum(direction * image)
            solution = solution + step_size * direction
            residual = residual - step_size * image
            if iteration + 1 < ITERS:
                scaled = residual / diagonal
                norm_next = jnp.sum(residual * scaled)
                direction = scaled + norm_next / norm_now * direction
                norm_now = norm_next
        return solution
    return lax.map(solve_one, (previous, dissipated))
```

```python
import functools
import math

import jax
import jax.numpy as jnp
from jax import lax
from jax.experimental import pallas as pl
from jax.experimental.pallas import tpu as pltpu
from jax.sharding import PartitionSpec as P

ITERS = 3
TIER_K = (1.0, 0.3, 0.12, 2.5)
CHANNEL_K = (1.0, 0.3, 0.25, 0.2)
CHANNEL_SINK = (0.0, 0.15, 0.45, 1.2)
TIER_HEAT = 0.05
CHANNEL_HEAT = 0.2
VERTICAL = 4.0

HALO = 8
STRIP = 4
SLOT = 2 * STRIP
MESH = pl.DeviceIdType.MESH

TIER_ROOT = tuple(math.sqrt(v) for v in TIER_K)
CHANNEL_ROOT = tuple(math.sqrt(v) for v in CHANNEL_K)
TIER_INV = tuple(1.0 / math.sqrt(v) for v in TIER_K)
CHANNEL_INV = tuple(1.0 / math.sqrt(v) for v in CHANNEL_K)


def lookup(codes, table):
    total = jnp.zeros(codes.shape, jnp.float32)
    for index, value in enumerate(table):
        total = jnp.where(codes == index, jnp.float32(value), total)
    return total


def coefficients(nu):
    def inner(a, b):
        total = None
        for i, x in enumerate(a):
            for j, y in enumerate(b):
                term = x * y * nu[i + j]
                total = term if total is None else total + term
        return total

    zero = nu[0] * 0.0
    rho = [zero + 1.0]
    pi = [zero + 1.0]
    norm = nu[0]
    result = [zero] * ITERS
    for iteration in range(ITERS):
        image = [a - b for a, b in zip(pi + [zero], [zero] + pi)]
        step = norm / inner(pi, image)
        for i, a in enumerate(pi):
            result[i] = result[i] + step * a
        if iteration + 1 < ITERS:
            rho = [a - step * b for a, b in zip(rho + [zero], image)]
            following = inner(rho, rho)
            growth = following / norm
            pi = [a + growth * b for a, b in zip(rho, pi + [zero])]
            norm = following
    return result


def kernel(nx, ny, prev, diss, mat, cool, out, vp, vq, vm, vc, own_l, own_r, far_l, far_r,
           edges, root, weight, capac, up, u0, u1, u2, result, row, rows,
           load_sem, send_sem, recv_sem, row_send, row_recv, store_sem):
    scen, layers, length, width = prev.shape
    tiers = mat.shape[0]
    n = nx * ny
    ext = length + 2 * HALO
    x, y = lax.axis_index("gx"), lax.axis_index("gy")
    me = x * ny + y
    barrier = pltpu.get_barrier_semaphore()

    def other(i):
        k = lax.rem(me + i, n)
        return k // ny, lax.rem(k, ny)

    def greet(i, carry):
        pl.semaphore_signal(barrier, inc=1, device_id=other(i), device_id_type=MESH)
        return carry

    inside = pl.ds(HALO, length)
    loads = [
        pltpu.make_async_copy(prev, vp.at[:, :, inside], load_sem.at[0]),
        pltpu.make_async_copy(diss, vq.at[:, :, inside], load_sem.at[1]),
        pltpu.make_async_copy(mat, vm.at[:, inside], load_sem.at[2]),
        pltpu.make_async_copy(cool, vc.at[:, inside], load_sem.at[3]),
    ]
    for copy in loads:
        copy.start()
    lax.fori_loop(1, n, greet, 0)

    has = {(-1, 0): x > 0, (1, 0): x < nx - 1, (0, -1): y > 0, (0, 1): y < ny - 1}
    for dx in (-1, 1):
        for dy in (-1, 1):
            has[dx, dy] = jnp.logical_and(has[dx, 0], has[0, dy])
    top, bottom = pl.ds(0, HALO), pl.ds(HALO + length, HALO)
    first, last = pl.ds(HALO, HALO), pl.ds(length, HALO)

    def fill(ref):
        ref[...] = jnp.full(ref.shape, -1, ref.dtype)

    for dx, where in ((-1, top), (1, bottom)):
        @pl.when(jnp.logical_not(has[dx, 0]))
        def _(where=where):
            for ref in (vp, vq):
                fill(ref.at[:, :, where])
            for ref in (vm, vc):
                fill(ref.at[:, where])
            fill(own_l.at[where])
            fill(own_r.at[where])
    for dy, ref in ((-1, far_l), (1, far_r)):
        @pl.when(jnp.logical_not(has[0, dy]))
        def _(ref=ref):
            fill(ref.at[inside])
        for dx, where in ((-1, top), (1, bottom)):
            @pl.when(jnp.logical_not(has[dx, dy]))
            def _(ref=ref, where=where):
                fill(ref.at[where])

    for copy in loads:
        copy.wait()

    places = []
    for s in range(scen):
        for layer in range(layers):
            places.append((SLOT * (s * layers + layer), vp, (s, layer)))
    for layer in range(layers):
        ref = vm if layer % 2 == 0 else vc
        places.append((SLOT * layer + STRIP, ref, (layer // 2,)))
    for t in range(tiers):
        places.append((SLOT * (layers + 1 + 2 * t) + STRIP, vq, (0, t)))
        places.append((SLOT * (layers + 2 * t) + STRIP, vq, (1, t)))
    chunk = 4 * HALO

    def pack(step, carry):
        start = pl.multiple_of(HALO + step * chunk, HALO)
        lane = lax.broadcasted_iota(jnp.int32, (chunk, width), 1)
        left = jnp.zeros((chunk, width), jnp.float32)
        right = jnp.zeros((chunk, width), jnp.float32)
        for base, ref, index in places:
            plane = ref[index + (pl.ds(start, chunk),)].astype(jnp.float32)
            turned = pltpu.roll(plane, base, 1) if base else plane
            left = jnp.where((lane >= base) & (lane < base + STRIP), turned, left)
            low = (base - STRIP) % width
            right = jnp.where((lane >= low) & (lane < low + STRIP), turned, right)
        own_l[pl.ds(start, chunk)] = left
        own_r[pl.ds(start, chunk)] = pltpu.roll(right, STRIP, 1)
        return carry

    lax.fori_loop(0, length // chunk, pack, 0)

    pl.semaphore_wait(barrier, n - 1)

    sends = []
    for dx, source, target in ((-1, first, bottom), (1, last, top)):
        for ref in (vp, vq):
            sends.append((dx, 0, ref.at[:, :, source], ref.at[:, :, target]))
        for ref in (vm, vc):
            sends.append((dx, 0, ref.at[:, source], ref.at[:, target]))
        for ref in (own_l, own_r):
            sends.append((dx, 0, ref.at[source], ref.at[target]))
        sends.append((dx, -1, own_l.at[source], far_r.at[target]))
        sends.append((dx, 1, own_r.at[source], far_l.at[target]))
    sends.append((0, -1, own_l.at[inside], far_r.at[inside]))
    sends.append((0, 1, own_r.at[inside], far_l.at[inside]))
    copies = []
    for i, (dx, dy, source, target) in enumerate(sends):
        copy = pltpu.make_async_remote_copy(
            src_ref=source, dst_ref=target, send_sem=send_sem.at[i], recv_sem=recv_sem.at[i],
            device_id=(x + dx, y + dy), device_id_type=MESH)
        copies.append((dx, dy, copy))
    order = sorted(copies, key=lambda c: 0 if c[0] == 0 else 1 if c[1] == 0 else 2)
    for dx, dy, copy in order:
        @pl.when(has[dx, dy])
        def _(copy=copy):
            copy.start()
    for dx, dy, copy in copies:
        @pl.when(has[-dx, -dy])
        def _(copy=copy):
            copy.wait_recv()

    shape = (ext, width)
    lane = lax.broadcasted_iota(jnp.int32, shape, 1)
    place = lane // SLOT
    low = lane % SLOT < STRIP
    layer_of = place % layers
    tier = layer_of % 2 == 0
    used = place < scen * layers

    def strip_stencil(u):
        lateral = pltpu.roll(u, 1, 1) + pltpu.roll(u, width - 1, 1)
        lateral = lateral + pltpu.roll(u, 1, 0) + pltpu.roll(u, ext - 1, 0)
        above = jnp.where(layer_of > 0, pltpu.roll(u, SLOT, 1), 0.0)
        below = jnp.where(layer_of < layers - 1, pltpu.roll(u, width - SLOT, 1), 0.0)
        return lateral + VERTICAL * (above + below)

    def strip(field, rest):
        codes = jnp.where(place < layers, rest, pltpu.roll(rest, SLOT * layers, 1))
        codes = jnp.where(used, codes, -1.0)
        power = jnp.where(place < layers, pltpu.roll(rest, width - SLOT * (layers + 1), 1), rest)
        power = jnp.where(tier & used, power, 0.0)
        s = jnp.where(tier, lookup(codes, TIER_ROOT), lookup(codes, CHANNEL_ROOT))
        heat = jnp.where(tier, TIER_HEAT, CHANNEL_HEAT)
        total = heat + jnp.where(tier, 0.0, lookup(codes, CHANNEL_SINK))
        total = total + s * strip_stencil(s)
        inverse = 1.0 / total
        scaled = s * field
        residual = (heat - total) * field + power + s * strip_stencil(scaled)
        w = s * s * inverse
        a = s * residual * inverse
        b = w * strip_stencil(a)
        c = w * strip_stencil(b)
        return s, scaled, a, b, c

    here, there = own_l[...], far_l[...]
    lefts = strip(jnp.where(low, there, pltpu.roll(here, STRIP, 1)),
                  jnp.where(low, pltpu.roll(there, width - STRIP, 1), here))
    for i, value in enumerate(lefts):
        edges[i] = value
    here, there = own_r[...], far_r[...]
    rights = strip(jnp.where(low, here, pltpu.roll(there, STRIP, 1)),
                   jnp.where(low, pltpu.roll(here, width - STRIP, 1), there))
    for i, value in enumerate(rights):
        edges[i] = jnp.where(lane % SLOT == STRIP - 1, edges[i], pltpu.roll(value, width - 2, 1))

    body = pl.ds(HALO, ext)
    blank = jnp.zeros((ext + 2 * HALO, width), jnp.float32)
    for pad in (0, layers + 1):
        root[pad] = blank
        for s in range(scen):
            for ref in (up, u0, u1, u2):
                ref[s, pad] = blank
    for layer in range(layers):
        if layer % 2 == 0:
            s = lookup(vm[layer // 2], TIER_ROOT)
            total = jnp.full(shape, TIER_HEAT, jnp.float32)
        else:
            codes = vc[layer // 2]
            s = lookup(codes, CHANNEL_ROOT)
            total = CHANNEL_HEAT + lookup(codes, CHANNEL_SINK)
        root[layer + 1, body] = s
        capac[layer] = total
        for k in range(scen):
            up[k, layer + 1, body] = s * vp[k, layer]

    def stencil(ref, at, layer, edge, slot):
        centre = ref[at + (layer + 1, body)]
        border = pltpu.roll(edges[edge], lax.rem(2 * width - STRIP + 1 - SLOT * slot, width), 1)
        west = jnp.where(lane == 0, border, pltpu.roll(centre, 1, 1))
        east = jnp.where(lane == width - 1, border, pltpu.roll(centre, width - 1, 1))
        lateral = west + east + ref[at + (layer + 1, pl.ds(HALO - 1, ext))]
        lateral = lateral + ref[at + (layer + 1, pl.ds(HALO + 1, ext))]
        vertical = ref[at + (layer, body)] + ref[at + (layer + 2, body)]
        return centre, lateral + VERTICAL * vertical

    def gather(total, value):
        tiles = value[HALO:HALO + length].reshape(length // HALO, HALO, width)
        return total + jnp.sum(tiles, axis=0)

    none = jnp.zeros((HALO, width), jnp.float32)

    def begin(layer, carry):
        is_tier = lax.rem(layer, 2) == 0
        heat = jnp.where(is_tier, jnp.float32(TIER_HEAT), jnp.float32(CHANNEL_HEAT))
        on = jnp.where(is_tier, jnp.float32(1.0), jnp.float32(0.0))
        s, around = stencil(root, (), layer, 0, layer)
        total = capac[layer] + s * around
        inverse = 1.0 / total
        weight[layer] = s * s * inverse
        sums = []
        for k in range(scen):
            _, around = stencil(up, (k,), layer, 1, k * layers + layer)
            residual = (heat - total) * vp[k, layer] + on * vq[k, layer // 2] + s * around
            scaled = residual * inverse
            u0[k, layer + 1, body] = s * scaled
            sums.append(gather(carry[k], residual * scaled))
        return tuple(sums)

    def advance(source, target, edge):
        def one(layer, carry):
            sums = []
            for k in range(scen):
                centre, around = stencil(source, (k,), layer, edge, k * layers + layer)
                sums.append(gather(carry[len(sums)], centre * around))
                if target is not None:
                    moved = weight[layer] * around
                    target[k, layer + 1, body] = moved
                    sums.append(gather(carry[len(sums)], moved * around))
            return tuple(sums)

        count = scen * (1 if target is None else 2)
        return lax.fori_loop(0, layers, one, (none,) * count)

    first_sums = lax.fori_loop(0, layers, begin, (none,) * scen)
    second = advance(u0, u1, 2)
    third = advance(u1, u2, 3)
    fourth = advance(u2, None, 4)
    moments = []
    for k in range(scen):
        moments += [first_sums[k], *second[2 * k:2 * k + 2], *third[2 * k:2 * k + 2], fourth[k]]
    count = len(moments)
    flat = jnp.zeros((1, width), jnp.float32)
    line = lax.broadcasted_iota(jnp.int32, (1, width), 1)
    for i, value in enumerate(moments):
        total = jnp.sum(jnp.sum(value, axis=0, keepdims=True), axis=1, keepdims=True)
        flat = jnp.where(line == i, total, flat)
    row[...] = flat
    rows[n - 1] = flat

    def to(i):
        return pltpu.make_async_remote_copy(
            src_ref=row, dst_ref=rows.at[i - 1], send_sem=row_send, recv_sem=row_recv,
            device_id=other(i), device_id_type=MESH)

    def spread(i, carry):
        to(i).start()
        return carry

    lax.fori_loop(1, n, spread, 0)
    for dx, dy, copy in copies:
        @pl.when(has[dx, dy])
        def _(copy=copy):
            copy.wait_send()
    arrived = rows.at[pl.ds(0, n - 1)]
    pltpu.make_async_copy(arrived, arrived, row_recv).wait()
    summed = jnp.sum(rows[...], axis=0)
    total = [jnp.sum(jnp.where(line == i, summed, 0.0), axis=1, keepdims=True)
             for i in range(count)]
    each = count // scen
    for k in range(scen):
        c0, c1, c2 = coefficients(total[k * each:(k + 1) * each])
        own = pl.ds(2 * HALO, length)
        for layer in range(layers):
            if layer % 2 == 0:
                back = lookup(vm[layer // 2, inside], TIER_INV)
            else:
                back = lookup(vc[layer // 2, inside], CHANNEL_INV)
            change = c0 * u0[k, layer + 1, own] + c1 * u1[k, layer + 1, own]
            change = change + c2 * u2[k, layer + 1, own]
            result[k, layer] = vp[k, layer, inside] + back * change
        pltpu.make_async_copy(result.at[k], out.at[k], store_sem.at[k]).start()
    for k in range(scen):
        pltpu.make_async_copy(result.at[k], out.at[k], store_sem.at[k]).wait()
    pltpu.make_async_copy(arrived, arrived, row_send).wait()


def per_device(nx, ny, previous, dissipated, material, coolant):
    scen, layers, length, width = previous.shape
    tiers = material.shape[0]
    ext = length + 2 * HALO
    f32 = jnp.float32
    field = pltpu.VMEM((scen, layers + 2, ext + 2 * HALO, width), f32)
    strip = pltpu.VMEM((ext, width), f32)
    return pl.pallas_call(
        functools.partial(kernel, nx, ny),
        out_shape=jax.ShapeDtypeStruct(previous.shape, f32),
        in_specs=[pl.BlockSpec(memory_space=pl.ANY)] * 4,
        out_specs=pl.BlockSpec(memory_space=pl.ANY),
        scratch_shapes=[
            pltpu.VMEM((scen, layers, ext, width), f32),
            pltpu.VMEM((scen, tiers, ext, width), f32),
            pltpu.VMEM((tiers, ext, width), jnp.int32),
            pltpu.VMEM((layers - tiers, ext, width), jnp.int32),
            strip, strip, strip, strip,
            pltpu.VMEM((5, ext, width), f32),
            pltpu.VMEM((layers + 2, ext + 2 * HALO, width), f32),
            pltpu.VMEM((layers, ext, width), f32),
            pltpu.VMEM((layers, ext, width), f32),
            field, field, field, field,
            pltpu.VMEM(previous.shape, f32),
            pltpu.VMEM((1, width), f32),
            pltpu.VMEM((nx * ny, 1, width), f32),
            pltpu.SemaphoreType.DMA((4,)),
            pltpu.SemaphoreType.DMA((18,)),
            pltpu.SemaphoreType.DMA((18,)),
            pltpu.SemaphoreType.DMA,
            pltpu.SemaphoreType.DMA,
            pltpu.SemaphoreType.DMA((scen,)),
        ],
        compiler_params=pltpu.CompilerParams(
            collective_id=0, has_side_effects=True, vmem_limit_bytes=40 * 1024 * 1024),
    )(previous, dissipated, material, coolant)


def solution(mesh):
    return jax.shard_map(
        functools.partial(per_device, mesh.shape["gx"], mesh.shape["gy"]),
        mesh=mesh,
        in_specs=(
            P(None, None, "gx", "gy"),
            P(None, None, "gx", "gy"),
            P(None, "gx", "gy"),
            P(None, "gx", "gy"),
        ),
        out_specs=P(None, None, "gx", "gy"),
        check_vma=False,
    )
```

```python
import functools
import math

import jax
import jax.numpy as jnp
from jax import lax
from jax.experimental import pallas as pl
from jax.experimental.pallas import tpu as pltpu
from jax.sharding import PartitionSpec as P

ITERS = 3
TIER_K = (1.0, 0.3, 0.12, 2.5)
CHANNEL_K = (1.0, 0.3, 0.25, 0.2)
CHANNEL_SINK = (0.0, 0.15, 0.45, 1.2)
TIER_HEAT = 0.05
CHANNEL_HEAT = 0.2
VERTICAL = 4.0

HALO = 8
STRIP = 4
SLOT = 2 * STRIP
MESH = pl.DeviceIdType.MESH

TIER_ROOT = tuple(math.sqrt(v) for v in TIER_K)
CHANNEL_ROOT = tuple(math.sqrt(v) for v in CHANNEL_K)
TIER_INV = tuple(1.0 / math.sqrt(v) for v in TIER_K)
CHANNEL_INV = tuple(1.0 / math.sqrt(v) for v in CHANNEL_K)


def lookup(codes, table):
    total = jnp.zeros(codes.shape, jnp.float32)
    for index, value in enumerate(table):
        total = jnp.where(codes == index, jnp.float32(value), total)
    return total


def coefficients(nu):
    def inner(a, b):
        total = None
        for i, x in enumerate(a):
            for j, y in enumerate(b):
                term = x * y * nu[i + j]
                total = term if total is None else total + term
        return total

    zero = nu[0] * 0.0
    rho = [zero + 1.0]
    pi = [zero + 1.0]
    norm = nu[0]
    result = [zero] * ITERS
    for iteration in range(ITERS):
        image = [a - b for a, b in zip(pi + [zero], [zero] + pi)]
        step = norm / inner(pi, image)
        for i, a in enumerate(pi):
            result[i] = result[i] + step * a
        if iteration + 1 < ITERS:
            rho = [a - step * b for a, b in zip(rho + [zero], image)]
            following = inner(rho, rho)
            growth = following / norm
            pi = [a + growth * b for a, b in zip(rho, pi + [zero])]
            norm = following
    return result


def kernel(nx, ny, prev, diss, mat, cool, out, vp, vq, vm, vc, own_l, own_r, far_l, far_r,
           edges, root, weight, capac, up, u0, u1, u2, result, row, rows,
           picks, split, load_sem, send_sem, recv_sem, row_send, row_recv, store_sem):
    scen, layers, length, width = prev.shape
    tiers = mat.shape[0]
    n = nx * ny
    ext = length + 2 * HALO
    x, y = lax.axis_index("gx"), lax.axis_index("gy")
    me = x * ny + y
    barrier = pltpu.get_barrier_semaphore()

    def other(i):
        k = lax.rem(me + i, n)
        return k // ny, lax.rem(k, ny)

    def greet(i, carry):
        pl.semaphore_signal(barrier, inc=1, device_id=other(i), device_id_type=MESH)
        return carry

    inside = pl.ds(HALO, length)
    loads = [
        pltpu.make_async_copy(prev, vp.at[:, :, inside], load_sem.at[0]),
        pltpu.make_async_copy(diss, vq.at[:, :, inside], load_sem.at[1]),
        pltpu.make_async_copy(mat, vm.at[:, inside], load_sem.at[2]),
        pltpu.make_async_copy(cool, vc.at[:, inside], load_sem.at[3]),
    ]
    for copy in loads:
        copy.start()
    lax.fori_loop(1, n, greet, 0)

    has = {(-1, 0): x > 0, (1, 0): x < nx - 1, (0, -1): y > 0, (0, 1): y < ny - 1}
    for dx in (-1, 1):
        for dy in (-1, 1):
            has[dx, dy] = jnp.logical_and(has[dx, 0], has[0, dy])
    top, bottom = pl.ds(0, HALO), pl.ds(HALO + length, HALO)
    first, last = pl.ds(HALO, HALO), pl.ds(length, HALO)

    def fill(ref):
        ref[...] = jnp.full(ref.shape, -1, ref.dtype)

    for dx, where in ((-1, top), (1, bottom)):
        @pl.when(jnp.logical_not(has[dx, 0]))
        def _(where=where):
            for ref in (vp, vq):
                fill(ref.at[:, :, where])
            for ref in (vm, vc):
                fill(ref.at[:, where])
            fill(own_l.at[where])
            fill(own_r.at[where])
    for dy, ref in ((-1, far_l), (1, far_r)):
        @pl.when(jnp.logical_not(has[0, dy]))
        def _(ref=ref):
            fill(ref.at[inside])
        for dx, where in ((-1, top), (1, bottom)):
            @pl.when(jnp.logical_not(has[dx, dy]))
            def _(ref=ref, where=where):
                fill(ref.at[where])

    for copy in loads:
        copy.wait()

    places = []
    for s in range(scen):
        for layer in range(layers):
            places.append((SLOT * (s * layers + layer), vp, (s, layer)))
    for layer in range(layers):
        ref = vm if layer % 2 == 0 else vc
        places.append((SLOT * layer + STRIP, ref, (layer // 2,)))
    for t in range(tiers):
        places.append((SLOT * (layers + 1 + 2 * t) + STRIP, vq, (0, t)))
        places.append((SLOT * (layers + 2 * t) + STRIP, vq, (1, t)))
    chunk = 4 * HALO

    def pack(step, carry):
        start = pl.multiple_of(HALO + step * chunk, HALO)
        lane = lax.broadcasted_iota(jnp.int32, (chunk, width), 1)
        left = jnp.zeros((chunk, width), jnp.float32)
        right = jnp.zeros((chunk, width), jnp.float32)
        for base, ref, index in places:
            plane = ref[index + (pl.ds(start, chunk),)].astype(jnp.float32)
            turned = pltpu.roll(plane, base, 1) if base else plane
            left = jnp.where((lane >= base) & (lane < base + STRIP), turned, left)
            low = (base - STRIP) % width
            right = jnp.where((lane >= low) & (lane < low + STRIP), turned, right)
        own_l[pl.ds(start, chunk)] = left
        own_r[pl.ds(start, chunk)] = pltpu.roll(right, STRIP, 1)
        return carry

    lax.fori_loop(0, length // chunk, pack, 0)

    def pick(slot, carry):
        near = (2 * width, width)
        source = lax.broadcasted_iota(jnp.int32, near, 0) % width - SLOT * slot
        target = lax.broadcasted_iota(jnp.int32, near, 1)
        west = (source == STRIP - 1) & (target == 0)
        east = (source == STRIP - 2) & (target == width - 1)
        picks[slot] = jnp.where(west | east, 1.0, 0.0).astype(jnp.bfloat16)
        return carry

    lax.fori_loop(0, scen * layers, pick, 0)

    pl.semaphore_wait(barrier, n - 1)

    sends = []
    for dx, source, target in ((-1, first, bottom), (1, last, top)):
        for ref in (vp, vq):
            sends.append((dx, 0, ref.at[:, :, source], ref.at[:, :, target]))
        for ref in (vm, vc):
            sends.append((dx, 0, ref.at[:, source], ref.at[:, target]))
        for ref in (own_l, own_r):
            sends.append((dx, 0, ref.at[source], ref.at[target]))
        sends.append((dx, -1, own_l.at[source], far_r.at[target]))
        sends.append((dx, 1, own_r.at[source], far_l.at[target]))
    sends.append((0, -1, own_l.at[inside], far_r.at[inside]))
    sends.append((0, 1, own_r.at[inside], far_l.at[inside]))
    copies = []
    for i, (dx, dy, source, target) in enumerate(sends):
        copy = pltpu.make_async_remote_copy(
            src_ref=source, dst_ref=target, send_sem=send_sem.at[i], recv_sem=recv_sem.at[i],
            device_id=(x + dx, y + dy), device_id_type=MESH)
        copies.append((dx, dy, copy))
    order = sorted(copies, key=lambda c: 0 if c[0] == 0 else 1 if c[1] == 0 else 2)
    for dx, dy, copy in order:
        @pl.when(has[dx, dy])
        def _(copy=copy):
            copy.start()
    blank = jnp.zeros((ext + 2 * HALO, width), jnp.float32)
    for pad in (0, layers + 1):
        root[pad] = blank
        for s in range(scen):
            for ref in (up, u0, u1, u2):
                ref[s, pad] = blank

    def prepare(begin, count):
        at, to = pl.ds(begin, count), pl.ds(begin + HALO, count)
        for layer in range(layers):
            if layer % 2 == 0:
                s = lookup(vm[layer // 2, at], TIER_ROOT)
                total = jnp.full((count, width), TIER_HEAT, jnp.float32)
            else:
                codes = vc[layer // 2, at]
                s = lookup(codes, CHANNEL_ROOT)
                total = CHANNEL_HEAT + lookup(codes, CHANNEL_SINK)
            root[layer + 1, to] = s
            capac[layer, at] = total
            for k in range(scen):
                up[k, layer + 1, to] = s * vp[k, layer, at]

    prepare(HALO, length)
    body = pl.ds(HALO, ext)

    def stencil(ref, at, layer, edge, slot, start=0, count=ext):
        lane = lax.broadcasted_iota(jnp.int32, (count, width), 1)
        rows_at = pl.ds(HALO + start, count)
        centre = ref[at + (layer + 1, rows_at)]
        west = jnp.where(lane == 0, 0.0, pltpu.roll(centre, 1, 1))
        east = jnp.where(lane == width - 1, 0.0, pltpu.roll(centre, width - 1, 1))
        lateral = west + east + ref[at + (layer + 1, pl.ds(HALO + start - 1, count))]
        lateral = lateral + ref[at + (layer + 1, pl.ds(HALO + start + 1, count))]
        vertical = ref[at + (layer, rows_at)] + ref[at + (layer + 2, rows_at)]
        around = lateral + VERTICAL * vertical
        if edge is not None:
            around = around + border(edge, slot, start, count)
        return centre, around

    def border(edge, slot, start, count):
        return jnp.dot(split[edge, pl.ds(start, count)], picks[slot],
                       preferred_element_type=jnp.float32)

    inner, rest = 2 * HALO, length - 2 * HALO

    def early(layer, carry):
        at = pl.ds(inner, rest)
        weight[layer, at] = stencil(root, (), layer, None, 0, inner, rest)[1]
        for k in range(scen):
            u1[k, layer + 1, at] = stencil(up, (k,), layer, None, 0, inner, rest)[1]
        return carry

    lax.fori_loop(0, layers, early, 0)

    for dx, dy, copy in copies:
        @pl.when(has[-dx, -dy])
        def _(copy=copy):
            copy.wait_recv()

    prepare(0, HALO)
    prepare(HALO + length, HALO)

    shape = (ext, width)
    lane = lax.broadcasted_iota(jnp.int32, shape, 1)
    place = lane // SLOT
    low = lane % SLOT < STRIP
    layer_of = place % layers
    tier = layer_of % 2 == 0
    used = place < scen * layers

    def strip_stencil(u):
        lateral = pltpu.roll(u, 1, 1) + pltpu.roll(u, width - 1, 1)
        lateral = lateral + pltpu.roll(u, 1, 0) + pltpu.roll(u, ext - 1, 0)
        above = jnp.where(layer_of > 0, pltpu.roll(u, SLOT, 1), 0.0)
        below = jnp.where(layer_of < layers - 1, pltpu.roll(u, width - SLOT, 1), 0.0)
        return lateral + VERTICAL * (above + below)

    def strip(field, rest):
        codes = jnp.where(place < layers, rest, pltpu.roll(rest, SLOT * layers, 1))
        codes = jnp.where(used, codes, -1.0)
        power = jnp.where(place < layers, pltpu.roll(rest, width - SLOT * (layers + 1), 1), rest)
        power = jnp.where(tier & used, power, 0.0)
        s = jnp.where(tier, lookup(codes, TIER_ROOT), lookup(codes, CHANNEL_ROOT))
        heat = jnp.where(tier, TIER_HEAT, CHANNEL_HEAT)
        total = heat + jnp.where(tier, 0.0, lookup(codes, CHANNEL_SINK))
        total = total + s * strip_stencil(s)
        inverse = 1.0 / total
        scaled = s * field
        residual = (heat - total) * field + power + s * strip_stencil(scaled)
        w = s * s * inverse
        a = s * residual * inverse
        b = w * strip_stencil(a)
        c = w * strip_stencil(b)
        return s, scaled, a, b, c

    here, there = own_l[...], far_l[...]
    lefts = strip(jnp.where(low, there, pltpu.roll(here, STRIP, 1)),
                  jnp.where(low, pltpu.roll(there, width - STRIP, 1), here))
    for i, value in enumerate(lefts):
        edges[i] = value
    here, there = own_r[...], far_r[...]
    rights = strip(jnp.where(low, here, pltpu.roll(there, STRIP, 1)),
                   jnp.where(low, pltpu.roll(here, width - STRIP, 1), there))
    for i, value in enumerate(rights):
        both = jnp.where(lane % SLOT == STRIP - 1, edges[i], pltpu.roll(value, width - 2, 1))
        high = both.astype(jnp.bfloat16)
        split[i, :, :width] = high
        split[i, :, width:] = (both - high.astype(jnp.float32)).astype(jnp.bfloat16)

    body = pl.ds(HALO, ext)

    def gather(total, value):
        tiles = value[HALO:HALO + length].reshape(length // HALO, HALO, width)
        return total + jnp.sum(tiles, axis=0)

    none = jnp.zeros((HALO, width), jnp.float32)

    def begin(layer, carry):
        is_tier = lax.rem(layer, 2) == 0
        heat = jnp.where(is_tier, jnp.float32(TIER_HEAT), jnp.float32(CHANNEL_HEAT))
        on = jnp.where(is_tier, jnp.float32(1.0), jnp.float32(0.0))
        sums = list(carry)
        for start, count in ((0, inner), (inner, rest), (inner + rest, inner)):
            at = pl.ds(start, count)
            if start == inner:
                s = root[layer + 1, pl.ds(HALO + start, count)]
                around = weight[layer, at] + border(0, layer, start, count)
            else:
                s, around = stencil(root, (), layer, 0, layer, start, count)
            total = capac[layer, at] + s * around
            inverse = 1.0 / total
            weight[layer, at] = s * s * inverse
            for k in range(scen):
                slot = k * layers + layer
                if start == inner:
                    around = u1[k, layer + 1, at] + border(1, slot, start, count)
                else:
                    _, around = stencil(up, (k,), layer, 1, slot, start, count)
                residual = (heat - total) * vp[k, layer, at] + on * vq[k, layer // 2, at]
                residual = residual + s * around
                scaled = residual * inverse
                u0[k, layer + 1, pl.ds(HALO + start, count)] = s * scaled
                own = residual * scaled
                own = own[HALO:] if start == 0 else own[:HALO] if start > inner else own
                sums[k] = sums[k] + jnp.sum(own.reshape(-1, HALO, width), axis=0)
        return tuple(sums)

    def advance(source, target, edge):
        def one(layer, carry):
            sums = []
            for k in range(scen):
                centre, around = stencil(source, (k,), layer, edge, k * layers + layer)
                sums.append(gather(carry[len(sums)], centre * around))
                if target is not None:
                    moved = weight[layer] * around
                    target[k, layer + 1, body] = moved
                    sums.append(gather(carry[len(sums)], moved * around))
            return tuple(sums)

        count = scen * (1 if target is None else 2)
        return lax.fori_loop(0, layers, one, (none,) * count, unroll=True)

    first_sums = lax.fori_loop(0, layers, begin, (none,) * scen, unroll=True)
    second = advance(u0, u1, 2)
    third = advance(u1, u2, 3)
    fourth = advance(u2, None, 4)
    moments = []
    for k in range(scen):
        moments += [first_sums[k], *second[2 * k:2 * k + 2], *third[2 * k:2 * k + 2], fourth[k]]
    count = len(moments)
    flat = jnp.zeros((1, width), jnp.float32)
    line = lax.broadcasted_iota(jnp.int32, (1, width), 1)
    for i, value in enumerate(moments):
        total = jnp.sum(jnp.sum(value, axis=0, keepdims=True), axis=1, keepdims=True)
        flat = jnp.where(line == i, total, flat)
    row[...] = flat
    rows[n - 1] = flat

    def to(i):
        return pltpu.make_async_remote_copy(
            src_ref=row, dst_ref=rows.at[i - 1], send_sem=row_send, recv_sem=row_recv,
            device_id=other(i), device_id_type=MESH)

    def spread(i, carry):
        to(i).start()
        return carry

    lax.fori_loop(1, n, spread, 0)
    for dx, dy, copy in copies:
        @pl.when(has[dx, dy])
        def _(copy=copy):
            copy.wait_send()
    own = pl.ds(2 * HALO, length)
    for layer in range(layers):
        if layer % 2 == 0:
            back = lookup(vm[layer // 2, inside], TIER_INV)
        else:
            back = lookup(vc[layer // 2, inside], CHANNEL_INV)
        for k in range(scen):
            for ref in (u0, u1, u2):
                ref[k, layer + 1, own] = back * ref[k, layer + 1, own]
    arrived = rows.at[pl.ds(0, n - 1)]
    pltpu.make_async_copy(arrived, arrived, row_recv).wait()
    summed = jnp.sum(rows[...], axis=0)
    total = [jnp.sum(jnp.where(line == i, summed, 0.0), axis=1, keepdims=True)
             for i in range(count)]
    each = count // scen
    for k in range(scen):
        c0, c1, c2 = coefficients(total[k * each:(k + 1) * each])
        for layer in range(layers):
            change = c0 * u0[k, layer + 1, own] + c1 * u1[k, layer + 1, own]
            change = change + c2 * u2[k, layer + 1, own]
            result[k, layer] = vp[k, layer, inside] + change
            pltpu.make_async_copy(result.at[k, layer], out.at[k, layer], store_sem).start()
    pltpu.make_async_copy(result, out, store_sem).wait()
    pltpu.make_async_copy(arrived, arrived, row_send).wait()


def per_device(nx, ny, previous, dissipated, material, coolant):
    scen, layers, length, width = previous.shape
    tiers = material.shape[0]
    ext = length + 2 * HALO
    f32 = jnp.float32
    field = pltpu.VMEM((scen, layers + 2, ext + 2 * HALO, width), f32)
    strip = pltpu.VMEM((ext, width), f32)
    return pl.pallas_call(
        functools.partial(kernel, nx, ny),
        out_shape=jax.ShapeDtypeStruct(previous.shape, f32),
        in_specs=[pl.BlockSpec(memory_space=pl.ANY)] * 4,
        out_specs=pl.BlockSpec(memory_space=pl.ANY),
        scratch_shapes=[
            pltpu.VMEM((scen, layers, ext, width), f32),
            pltpu.VMEM((scen, tiers, ext, width), f32),
            pltpu.VMEM((tiers, ext, width), jnp.int32),
            pltpu.VMEM((layers - tiers, ext, width), jnp.int32),
            strip, strip, strip, strip,
            pltpu.VMEM((5, ext, width), f32),
            pltpu.VMEM((layers + 2, ext + 2 * HALO, width), f32),
            pltpu.VMEM((layers, ext, width), f32),
            pltpu.VMEM((layers, ext, width), f32),
            field, field, field, field,
            pltpu.VMEM(previous.shape, f32),
            pltpu.VMEM((1, width), f32),
            pltpu.VMEM((nx * ny, 1, width), f32),
            pltpu.VMEM((scen * layers, 2 * width, width), jnp.bfloat16),
            pltpu.VMEM((5, ext, 2 * width), jnp.bfloat16),
            pltpu.SemaphoreType.DMA((4,)),
            pltpu.SemaphoreType.DMA((18,)),
            pltpu.SemaphoreType.DMA((18,)),
            pltpu.SemaphoreType.DMA,
            pltpu.SemaphoreType.DMA,
            pltpu.SemaphoreType.DMA,
        ],
        compiler_params=pltpu.CompilerParams(
            collective_id=0, has_side_effects=True, vmem_limit_bytes=56 * 1024 * 1024),
    )(previous, dissipated, material, coolant)


def solution(mesh):
    return jax.shard_map(
        functools.partial(per_device, mesh.shape["gx"], mesh.shape["gy"]),
        mesh=mesh,
        in_specs=(
            P(None, None, "gx", "gy"),
            P(None, None, "gx", "gy"),
            P(None, "gx", "gy"),
            P(None, "gx", "gy"),
        ),
        out_specs=P(None, None, "gx", "gy"),
        check_vma=False,
    )
```
